128 devices in a mesh: row: 8 (over z, y_hi), col: 16 (over x, y_lo, core).
Axes of the slice: x: 4, y: 4 (y_hi: 2, y_lo: 2; y = y_hi * 2 + y_lo), z: 4, core: 2. Of those that a mesh axis runs over, the one named last changes fastest.
Arguments:
- tri_panels: float32 [8192, 8192], P('row', 'col'), may hold values from -1 to 2, as said below
- rhs_rows: float32 [8192, 2048], P(('row', 'col')), may hold values from -6 to 6
Outputs:
- rhs_grid: float32 [8192, 2048], P('row', 'col')
The draws below stay inside these ranges and needn't reach their ends.
Inputs may be any that keep to these rules, and one draw needn't show every extreme that they name: `tri_panels`: in L's row order the entries above the diagonal are zero and the diagonal entries are positive.
All inputs are finite; a program needn't handle non-finite values.
Results may differ from the reference program's by a relative error of at most 0.00011.
Values sent between devices are 32-bit elements; how exact they have to be, the bound alone decides.
No kernel may reach another device: no remote copies, remote signals or barrier semaphores. Data moves between devices by JAX's collectives and lax.ppermute only.
A program may use at most 256 MiB of HBM per device.

```python
import math
import jax
import jax.numpy as jnp
from jax import lax

N = 8192
NB = 512
NRHS = 2048
K = 8192
N_ROW = 8
N_COL = 16


def draw_tri_panels(key, part):
    key_offdiag = jax.random.fold_in(key, 11)
    key_diagonal = jax.random.fold_in(key, 23)
    bound_value = 2.7 / math.sqrt(N)
    off_diagonal = jax.random.uniform(key_offdiag, (N, K), jnp.float32, -bound_value, bound_value)
    diagonal_values = jnp.exp(jax.random.uniform(key_diagonal, (N,), jnp.float32, 0.0, math.log(2.0)))
    row_index = jnp.arange(N, dtype=jnp.int32)[:, None]
    col_index = jnp.arange(K, dtype=jnp.int32)[None, :]
    matrix_lower = jnp.where(row_index > col_index, off_diagonal, jnp.float32(0.0))
    matrix_lower = jnp.where(row_index == col_index, diagonal_values[:, None], matrix_lower)
    block_count = N // (N_ROW * NB)
    return matrix_lower.reshape(block_count, N_ROW, NB, K).transpose(1, 0, 2, 3).reshape(N, K)


def level_of(rng, shape, cuts, least, high):
    def one(axis_at, parts):
        steps = jax.random.uniform(jax.random.fold_in(jax.random.fold_in(rng, 6), axis_at), (parts,), jnp.float32, least / len(cuts), high / len(cuts))
        return jnp.repeat(jnp.exp(steps), shape[axis_at] // parts).reshape((-1,) + (1,) * (len(shape) - axis_at - 1))

    gain = one(*cuts[0])
    for cut in cuts[1:]:
        gain = gain * one(*cut)
    return gain


def normal_values(key, extent, deviation, most, pieces=(), kind=jnp.bfloat16):
    factor_of = level_of(key, extent, pieces, -0.22, 0.18) if pieces else 1.0
    drawn = jax.random.normal(key, extent, jnp.float32) * deviation * factor_of
    return jnp.minimum(jnp.maximum(drawn, -most), most).astype(kind)


def setup_inputs(seed: int = 0) -> dict:
    splits = jax.random.split(jax.random.key(seed), 3)
    return {
        "tri_panels": draw_tri_panels(jax.random.fold_in(splits[2], 71), 0),
        "rhs_rows": normal_values(splits[1], (N, NRHS), 1.0, 6.0, ((0, 128),), jnp.float32),
    }


def reference(tri_panels, rhs_rows):
    block_count = N // (N_ROW * NB)
    sub_rows = NB // N_COL
    lower_full = tri_panels.reshape(N_ROW, block_count, NB, K).transpose(1, 0, 2, 3).reshape(N, K)
    right_side = rhs_rows.reshape(N_ROW, N_COL, block_count, sub_rows, NRHS).transpose(2, 0, 1, 3, 4).reshape(N, NRHS)
    for step_index in range(N_COL):
        top_row = step_index * NB
        bottom = top_row + NB
        solution = jax.scipy.linalg.solve_triangular(lower_full[top_row:bottom, top_row:bottom], right_side[top_row:bottom], lower=True)
        below_rows = right_side[bottom:] - jnp.dot(lower_full[bottom:, top_row:bottom].astype(jnp.float32), solution.astype(jnp.float32), precision=lax.Precision.HIGHEST, preferred_element_type=jnp.float32)
        right_side = jnp.concatenate([right_side[:top_row], solution, below_rows], 0)
    return right_side.reshape(block_count, N_ROW, NB, NRHS).transpose(1, 0, 2, 3).reshape(N, NRHS)
```

```python
import jax
import jax.numpy as jnp
from jax import lax
from jax.sharding import PartitionSpec as P

HI = lax.Precision.HIGHEST


def mm(a, b):
    return jnp.dot(a, b, precision=HI, preferred_element_type=jnp.float32)


def on_device(tri_panels, rhs_rows):
    R = lax.axis_size("row")
    C = lax.axis_size("col")
    p = lax.axis_index("row")
    c = lax.axis_index("col")
    nb = tri_panels.shape[1]
    half = nb // 2
    blocks = tri_panels.shape[0] // nb
    sub = nb // C
    width = rhs_rows.shape[1] // C
    parted = rhs_rows.reshape(blocks, sub, rhs_rows.shape[1])
    state = lax.all_to_all(parted, "col", split_axis=2, concat_axis=1, tiled=True)

    eye = jnp.eye(nb, dtype=jnp.float32)
    own = tri_panels.reshape(blocks, nb, nb)
    is_diag = c % R == p
    diag = lax.dynamic_index_in_dim(own, c // R, 0, keepdims=False)
    diag = jnp.where(is_diag, diag, eye)
    inv = jax.scipy.linalg.solve_triangular(diag, eye, lower=True)
    top = jnp.where(is_diag & (c < R), inv, own[0])
    low = jnp.where(is_diag & (c >= R), inv, own[1])

    moved = lax.ppermute(top[half:], "col", [(i, i + R) for i in range(R)])
    piece = jnp.where(c < R, top[:half], moved)
    g0 = lax.all_gather(piece, "col", axis=0, tiled=False).reshape(2, R, half, nb)
    g1 = lax.all_gather(low, "col", axis=0, tiled=False)

    def block0(k):
        k = jnp.clip(k, 0, R - 1)
        return lax.dynamic_index_in_dim(g0, k, 1, keepdims=False).reshape(nb, nb)

    def block1(k):
        k = jnp.clip(k, 0, C - 1)
        return lax.dynamic_index_in_dim(g1, k, 0, keepdims=False)

    acc0, acc1 = state[0], state[1]
    inv0 = block0(p)
    near0 = mm(inv0, block0(p - 1))
    inv1 = None
    zero = jnp.zeros((nb, width), jnp.float32)
    store = jnp.zeros((R + 1, nb, width), jnp.float32)
    C0 = mm(inv0, acc0)
    mine = jnp.where(p == 0, C0, zero)
    out0 = mine
    C1 = None
    for t in range(C - 1):
        s = t % R
        with jax.named_scope(f"near{t}"):
            P1 = lax.ppermute(mine, "row", [(s, (s + 1) % R)])
        B = [((t - j) % R, (t + 2 + j) % R) for j in range(3) if t - j >= 0 and t + 2 + j < C]
        A = [((t - j) % R, (t + 1 + j) % R) for j in range(1, 4) if t - j >= 0 and t + 1 + j < C]
        XB = XA = None
        with jax.named_scope(f"far{t}"):
            if B:
                XB = lax.ppermute(mine, "row", B)
            if A:
                XA = lax.ppermute(mine, "row", A)
        q = (p - t) % R
        i = t + q
        kA = i - 2 * q + 1
        kB = kA + 1
        inwin = (q >= 2) & (q <= 4)
        if t + 1 < R:
            xc = C0 - mm(near0, P1)
            mine = jnp.where(p == t + 1, xc, mine)
            out0 = mine
            if t > 0:
                pass
            if XB is not None:
                store = lax.dynamic_update_index_in_dim(store, XB, jnp.where(inwin & (kB >= 0), kB, R), 0)
                acc0 = acc0 - mm(block0(kB), XB)
            if XA is not None:
                store = lax.dynamic_update_index_in_dim(store, XA, jnp.where(inwin & (kA >= 0), kA, R), 0)
                acc0 = acc0 - mm(block0(kA), XA)
            store = lax.dynamic_update_index_in_dim(store, P1, jnp.where(p == t + 1, t, R), 0)
            C0 = mm(inv0, acc0)
            if t + 1 == R - 1:
                store = lax.dynamic_update_index_in_dim(store, mine, p, 0)
                inv1 = block1(R + p)
                near1 = mm(inv1, block1(R + p - 1))
                prod = jnp.zeros((nb, width), jnp.float32)
                for k in range(R):
                    prod = prod + mm(g1[k], store[k])
                acc1 = acc1 - prod
                C1 = mm(inv1, acc1)
        else:
            xc = C1 - mm(near1, P1)
            mine = jnp.where(p == (t + 1) - R, xc, mine)
            if XB is not None:
                acc1 = acc1 - mm(block1(kB), XB)
            if XA is not None:
                acc1 = acc1 - mm(block1(kA), XA)
            C1 = mm(inv1, acc1)
    return jnp.concatenate([out0, mine], 0)


def solution(mesh):
    return jax.shard_map(
        on_device,
        mesh=mesh,
        in_specs=(P("row", "col"), P(("row", "col"), None)),
        out_specs=P("row", "col"),
        check_vma=False,
    )
```

```python
import jax
import jax.numpy as jnp
from jax import lax
from jax.experimental import pallas as pl
from jax.experimental.pallas import tpu as pltpu
from jax.sharding import PartitionSpec as P

F32 = jnp.float32
BF16 = jnp.bfloat16
VMEM = pltpu.VMEM
SMEM = pltpu.SMEM
TILE = 128


def split(x):
    hi = x.astype(BF16)
    lo = (x - hi.astype(F32)).astype(BF16)
    return hi, lo


def left3(x):
    hi, lo = split(x)
    return jnp.concatenate([hi, hi, lo], 1)


def right3(x):
    hi, lo = split(x)
    return jnp.concatenate([hi, lo, hi], 0)


def dot3(a3, b3):
    return jnp.dot(a3, b3, preferred_element_type=F32)


def mm3(a, b):
    return dot3(left3(a), right3(b))


def vspec():
    return pl.BlockSpec(memory_space=VMEM)


def sspec():
    return pl.BlockSpec(memory_space=SMEM)


def aspec():
    return pl.BlockSpec(memory_space=pl.ANY)


PARAMS = pltpu.CompilerParams(vmem_limit_bytes=48 * 1024 * 1024)


def rows_loop(n, body):
    lax.fori_loop(0, n // TILE, lambda r, _: (body(pl.ds(pl.multiple_of(r * TILE, TILE), TILE)), 0)[1], 0)


def inverse_kernel(flag, own, out):
    nb = own.shape[1]
    h = nb // 2
    out[...] = own[...]

    def invert(slot):
        row = lax.broadcasted_iota(jnp.int32, (h, h), 0)
        col = lax.broadcasted_iota(jnp.int32, (h, h), 1)
        a0 = own[slot, :h, :h]
        a1 = own[slot, h:, h:]
        on = row == col
        y0 = jnp.where(on, 1.0 / jnp.where(on, a0, 1.0), 0.0)
        y1 = jnp.where(on, 1.0 / jnp.where(on, a1, 1.0), 0.0)

        def level(n, ys):
            y0, y1 = ys
            s = lax.shift_left(jnp.int32(1), n)
            pick = (lax.shift_right_logical(row, n + 1) == lax.shift_right_logical(col, n + 1))
            pick = pick & ((row & s) != 0) & ((col & s) == 0)
            e0 = jnp.where(pick, a0, 0.0)
            e1 = jnp.where(pick, a1, 0.0)
            z0 = mm3(e0, y0)
            z1 = mm3(e1, y1)
            return y0 - mm3(y0, z0), y1 - mm3(y1, z1)

        steps = h.bit_length() - 1
        y0, y1 = lax.fori_loop(0, steps, level, (y0, y1))
        z = mm3(own[slot, h:, :h], y0)
        out[slot, :h, :h] = y0
        out[slot, h:, h:] = y1
        out[slot, h:, :h] = -mm3(y1, z)
        out[slot, :h, h:] = jnp.zeros((h, h), F32)

    @pl.when(flag[0] > 0)
    def _():
        invert(flag[1])


def inverse_call(flag, own):
    return pl.pallas_call(
        inverse_kernel,
        out_shape=jax.ShapeDtypeStruct(own.shape, F32),
        in_specs=[sspec(), vspec()],
        out_specs=vspec(),
        compiler_params=PARAMS,
        name="inverse",
    )(flag, own)


def fetch(g, k, buf, sem):
    parts, _, rows, _ = g.shape
    return [
        pltpu.make_async_copy(g.at[a, k], buf.at[pl.ds(a * rows, rows)], sem.at[a])
        for a in range(parts)
    ]


def prep_kernel(idx, g, acc, inv3, near3, cur, b0, b1, s0, s1):
    c0 = fetch(g, idx[0], b0, s0)
    c1 = fetch(g, idx[1], b1, s1)
    for x in c0 + c1:
        x.start()
    for x in c0:
        x.wait()

    def put(ds):
        inv3[ds] = left3(b0[ds])

    rows_loop(b0.shape[0], put)
    for x in c1:
        x.wait()
    l3 = right3(b1[...])
    a3 = right3(acc[...])

    def mul(ds):
        near3[ds] = left3(dot3(inv3[ds], l3))
        cur[ds] = dot3(inv3[ds], a3)

    rows_loop(b0.shape[0], mul)


def prep_call(idx, g, acc):
    nb, width = acc.shape
    parts = g.shape[0]
    return pl.pallas_call(
        prep_kernel,
        out_shape=(
            jax.ShapeDtypeStruct((nb, 3 * nb), BF16),
            jax.ShapeDtypeStruct((nb, 3 * nb), BF16),
            jax.ShapeDtypeStruct((nb, width), F32),
        ),
        in_specs=[sspec(), aspec(), vspec()],
        out_specs=(vspec(), vspec(), vspec()),
        scratch_shapes=[
            VMEM((nb, nb), F32),
            VMEM((nb, nb), F32),
            pltpu.SemaphoreType.DMA((parts,)),
            pltpu.SemaphoreType.DMA((parts,)),
        ],
        compiler_params=PARAMS,
        name="prep",
    )(idx, g, acc)


def near_kernel(flag, near3, got, cur, mine, out):
    @pl.when(flag[0] > 0)
    def _():
        x3 = right3(got[...])

        def mul(ds):
            out[ds] = cur[ds] - dot3(near3[ds], x3)

        rows_loop(out.shape[0], mul)

    @pl.when(flag[0] == 0)
    def _():
        out[...] = mine[...]


def near_call(flag, near3, got, cur, mine):
    return pl.pallas_call(
        near_kernel,
        out_shape=jax.ShapeDtypeStruct(mine.shape, F32),
        in_specs=[sspec(), vspec(), vspec(), vspec(), vspec()],
        out_specs=vspec(),
        compiler_params=PARAMS,
        name="near",
    )(flag, near3, got, cur, mine)


def far_kernel(idx, g, inv3, acc, xb, xa, acc_out, cur_out, b0, b1, s0, s1):
    @pl.when(idx[2] > 0)
    def _():
        c0 = fetch(g, idx[0], b0, s0)
        c1 = fetch(g, idx[1], b1, s1)
        for x in c0 + c1:
            x.start()
        xb3 = right3(xb[...])
        xa3 = right3(xa[...])
        for x in c0 + c1:
            x.wait()

        def mul(ds):
            acc_out[ds] = acc[ds] - (dot3(left3(b0[ds]), xb3) + dot3(left3(b1[ds]), xa3))

        rows_loop(acc.shape[0], mul)
        a3 = right3(acc_out[...])

        def mul2(ds):
            cur_out[ds] = dot3(inv3[ds], a3)

        rows_loop(acc.shape[0], mul2)

    @pl.when(idx[2] == 0)
    def _():
        acc_out[...] = acc[...]
        cur_out[...] = acc[...]


def far_call(idx, g, inv3, acc, xb, xa):
    nb = acc.shape[0]
    parts = g.shape[0]
    return pl.pallas_call(
        far_kernel,
        out_shape=(
            jax.ShapeDtypeStruct(acc.shape, F32),
            jax.ShapeDtypeStruct(acc.shape, F32),
        ),
        in_specs=[sspec(), aspec(), vspec(), vspec(), vspec(), vspec()],
        out_specs=(vspec(), vspec()),
        scratch_shapes=[
            VMEM((nb, nb), F32),
            VMEM((nb, nb), F32),
            pltpu.SemaphoreType.DMA((parts,)),
            pltpu.SemaphoreType.DMA((parts,)),
        ],
        compiler_params=PARAMS,
        name="far",
    )(idx, g, inv3, acc, xb, xa)


def bulk_kernel(g, store, acc, out):
    k = pl.program_id(0)

    @pl.when(k == 0)
    def _():
        out[...] = acc[...]

    x3 = right3(store[0])

    def mul(ds):
        out[ds] = out[ds] - dot3(left3(g[0, 0, ds]), x3)

    rows_loop(out.shape[0], mul)


def bulk_call(g, store, acc, count):
    nb, width = acc.shape
    return pl.pallas_call(
        bulk_kernel,
        out_shape=jax.ShapeDtypeStruct(acc.shape, F32),
        grid=(count,),
        in_specs=[
            pl.BlockSpec((1, 1, nb, nb), lambda k: (0, k, 0, 0)),
            pl.BlockSpec((1, nb, width), lambda k: (k, 0, 0)),
            pl.BlockSpec((nb, width), lambda k: (0, 0)),
        ],
        out_specs=pl.BlockSpec((nb, width), lambda k: (0, 0)),
        compiler_params=PARAMS,
        name="bulk",
    )(g, store, acc)


def on_device(tri_panels, rhs_rows):
    R = lax.axis_size("row")
    C = lax.axis_size("col")
    p = lax.axis_index("row")
    c = lax.axis_index("col")
    nb = tri_panels.shape[1]
    half = nb // 2
    blocks = tri_panels.shape[0] // nb
    sub = nb // C
    width = rhs_rows.shape[1] // C
    parted = rhs_rows.reshape(blocks, sub, rhs_rows.shape[1])
    state = lax.all_to_all(parted, "col", split_axis=2, concat_axis=1, tiled=True)

    own = tri_panels.reshape(blocks, nb, nb)
    flag = jnp.stack([(c % R == p).astype(jnp.int32), c // R])
    own = inverse_call(flag, own)
    top, low = own[0], own[1]

    moved = lax.ppermute(top[half:], "col", [(i, i + R) for i in range(R)])
    piece = jnp.where(c < R, top[:half], moved)
    g0 = lax.all_gather(piece, "col", axis=0, tiled=False).reshape(2, R, half, nb)
    g1 = lax.all_gather(low, "col", axis=0, tiled=False).reshape(1, C, nb, nb)

    def ints(*v):
        return jnp.stack([jnp.asarray(x, jnp.int32) for x in v])

    acc0, acc1 = state[0], state[1]
    inv0, near0, cur0 = prep_call(ints(p, jnp.maximum(p - 1, 0)), g0, acc0)
    zero = jnp.zeros((nb, width), F32)
    store = jnp.zeros((R + 1, nb, width), F32)
    mine = jnp.where(p == 0, cur0, zero)
    out0 = mine
    for t in range(C - 1):
        s = t % R
        with jax.named_scope(f"near{t}"):
            P1 = lax.ppermute(mine, "row", [(s, (s + 1) % R)])
        B = [((t - j) % R, (t + 2 + j) % R) for j in range(3) if t - j >= 0 and t + 2 + j < C]
        A = [((t - j) % R, (t + 1 + j) % R) for j in range(1, 4) if t - j >= 0 and t + 1 + j < C]
        with jax.named_scope(f"far{t}"):
            XB = lax.ppermute(mine, "row", B) if B else zero
            XA = lax.ppermute(mine, "row", A) if A else zero
        q = (p - t) % R
        i = t + q
        kA = i - 2 * q + 1
        kB = kA + 1
        inwin = (q >= 2) & (q <= 4)
        first = t + 1 < R
        fi = ints(
            jnp.clip(kB, 0, R - 1 if first else C - 1),
            jnp.clip(kA, 0, R - 1 if first else C - 1),
            inwin,
        )
        turn = ints(p == (t + 1) % R)
        if first:
            mine = near_call(turn, near0, P1, cur0, mine)
            out0 = mine
            if B:
                store = lax.dynamic_update_index_in_dim(store, XB, jnp.where(inwin & (kB >= 0), kB, R), 0)
            if A:
                store = lax.dynamic_update_index_in_dim(store, XA, jnp.where(inwin & (kA >= 0), kA, R), 0)
            store = lax.dynamic_update_index_in_dim(store, P1, jnp.where(p == t + 1, t, R), 0)
            if t + 1 < R - 1:
                acc0, cur0 = far_call(fi, g0, inv0, acc0, XB, XA)
            else:
                store = lax.dynamic_update_index_in_dim(store, mine, p, 0)
                acc1 = bulk_call(g1, store, acc1, R)
                inv1, near1, cur1 = prep_call(ints(R + p, R + p - 1), g1, acc1)
        else:
            mine = near_call(turn, near1, P1, cur1, mine)
            if B or A:
                acc1, cur1 = far_call(fi, g1, inv1, acc1, XB, XA)
    return jnp.concatenate([out0, mine], 0)


def solution(mesh):
    return jax.shard_map(
        on_device,
        mesh=mesh,
        in_specs=(P("row", "col"), P(("row", "col"), None)),
        out_specs=P("row", "col"),
        check_vma=False,
    )
```

```python
import jax
import jax.numpy as jnp
from jax import lax
from jax.experimental import pallas as pl
from jax.experimental.pallas import tpu as pltpu
from jax.sharding import PartitionSpec as P

F32 = jnp.float32
BF16 = jnp.bfloat16
VMEM = pltpu.VMEM
SMEM = pltpu.SMEM
TILE = 256


def split(x):
    hi = x.astype(BF16)
    lo = (x - hi.astype(F32)).astype(BF16)
    return hi, lo


def left3(x):
    hi, lo = split(x)
    return jnp.concatenate([hi, hi, lo], 1)


def right3(x):
    hi, lo = split(x)
    return jnp.concatenate([hi, lo, hi], 0)


def mm3(a, b):
    return jnp.dot(left3(a), right3(b), preferred_element_type=F32)


def wide(x):
    return jnp.concatenate(split(x), 1)


def mmw(hi, lo, w):
    r = jnp.dot(hi, w, preferred_element_type=F32) + jnp.dot(lo, w, preferred_element_type=F32)
    n = w.shape[1] // 2
    return r[:, :n] + r[:, n:]


def vspec():
    return pl.BlockSpec(memory_space=VMEM)


def sspec():
    return pl.BlockSpec(memory_space=SMEM)


def aspec():
    return pl.BlockSpec(memory_space=pl.ANY)


PARAMS = pltpu.CompilerParams(vmem_limit_bytes=48 * 1024 * 1024)


def rows_loop(n, body, tile=TILE):
    lax.fori_loop(0, n // tile, lambda r, _: (body(pl.ds(pl.multiple_of(r * tile, tile), tile)), 0)[1], 0)


def inverse_kernel(flag, own, out):
    nb = own.shape[1]
    h = nb // 2
    out[...] = own[...]

    def invert(slot):
        row = lax.broadcasted_iota(jnp.int32, (h, h), 0)
        col = lax.broadcasted_iota(jnp.int32, (h, h), 1)
        a0 = own[slot, :h, :h]
        a1 = own[slot, h:, h:]
        on = row == col
        y0 = jnp.where(on, 1.0 / jnp.where(on, a0, 1.0), 0.0)
        y1 = jnp.where(on, 1.0 / jnp.where(on, a1, 1.0), 0.0)

        def level(n, ys):
            y0, y1 = ys
            s = lax.shift_left(jnp.int32(1), n)
            pick = (lax.shift_right_logical(row, n + 1) == lax.shift_right_logical(col, n + 1))
            pick = pick & ((row & s) != 0) & ((col & s) == 0)
            e0 = jnp.where(pick, a0, 0.0)
            e1 = jnp.where(pick, a1, 0.0)
            z0 = mm3(e0, y0)
            z1 = mm3(e1, y1)
            return y0 - mm3(y0, z0), y1 - mm3(y1, z1)

        steps = h.bit_length() - 1
        y0, y1 = lax.fori_loop(0, steps, level, (y0, y1))
        z = mm3(own[slot, h:, :h], y0)
        out[slot, :h, :h] = y0
        out[slot, h:, h:] = y1
        out[slot, h:, :h] = -mm3(y1, z)
        out[slot, :h, h:] = jnp.zeros((h, h), F32)

    @pl.when(flag[0] > 0)
    def _():
        invert(flag[1])


def inverse_call(flag, own):
    return pl.pallas_call(
        inverse_kernel,
        out_shape=jax.ShapeDtypeStruct(own.shape, F32),
        in_specs=[sspec(), vspec()],
        out_specs=vspec(),
        compiler_params=PARAMS,
        name="inverse",
    )(flag, own)


class Panels:
    def __init__(self, table, parts):
        self.arrays = [a for pos in table for a in pos]
        self.counts = [len(pos) for pos in table]
        self.parts = parts

    def specs(self):
        return [aspec() for _ in self.arrays]

    def start(self, refs, pos, dst, sem):
        at = []
        n = 0
        for m in self.counts:
            at.append(refs[n : n + m])
            n += m
        for static in range(len(self.counts)):
            def go(static=static):
                row = 0
                for half in range(self.parts):
                    for r in at[static ^ (8 * half)]:
                        pltpu.make_async_copy(r, dst.at[pl.ds(row, r.shape[0])], sem).start()
                        row += r.shape[0]

            pl.when(pos == static)(go)


def arrived(dst, sem):
    pltpu.make_async_copy(dst, dst, sem).wait()


def prep_call(g, idx, acc):
    nb, width = acc.shape
    m = len(g.arrays)

    def kernel(idx, acc, *rest):
        refs = rest[:m]
        invh, invl, nearh, nearl, cur, b0, b1, sem = rest[m:]
        g.start(refs, idx[0], b0, sem.at[0])
        g.start(refs, idx[1], b1, sem.at[1])
        arrived(b0, sem.at[0])

        def put(ds):
            invh[ds], invl[ds] = split(b0[ds])

        rows_loop(nb, put)
        w = wide(acc[...])

        def mul(ds):
            cur[ds] = mmw(invh[ds], invl[ds], w)

        rows_loop(nb, mul)
        arrived(b1, sem.at[1])
        lw = wide(b1[...])

        def mul2(ds):
            nearh[ds], nearl[ds] = split(mmw(invh[ds], invl[ds], lw))

        rows_loop(nb, mul2)

    sq = jax.ShapeDtypeStruct((nb, nb), BF16)
    return pl.pallas_call(
        kernel,
        out_shape=(sq, sq, sq, sq, jax.ShapeDtypeStruct((nb, width), F32)),
        in_specs=[sspec(), vspec()] + g.specs(),
        out_specs=(vspec(),) * 5,
        scratch_shapes=[VMEM((nb, nb), F32), VMEM((nb, nb), F32), pltpu.SemaphoreType.DMA((2,))],
        compiler_params=PARAMS,
        name="prep",
    )(idx, acc, *g.arrays)


def pick_call(g, idx, nb):
    m = len(g.arrays)

    def kernel(idx, *rest):
        refs = rest[:m]
        hi, lo, b0, b1, sem = rest[m:]

        @pl.when(idx[2] > 0)
        def _():
            g.start(refs, idx[0], b0, sem.at[0])
            g.start(refs, idx[1], b1, sem.at[1])
            for n, b in enumerate((b0, b1)):
                arrived(b, sem.at[n])

                def put(ds):
                    hi[ds, n * nb : (n + 1) * nb], lo[ds, n * nb : (n + 1) * nb] = split(b[ds])

                rows_loop(nb, put, 64)

    out = jax.ShapeDtypeStruct((nb, 2 * nb), BF16)
    return pl.pallas_call(
        kernel,
        out_shape=(out, out),
        in_specs=[sspec()] + g.specs(),
        out_specs=(vspec(), vspec()),
        scratch_shapes=[VMEM((nb, nb), F32), VMEM((nb, nb), F32), pltpu.SemaphoreType.DMA((2,))],
        compiler_params=PARAMS,
        name="pick",
    )(idx, *g.arrays)


def near_call(flag, nearh, nearl, got, cur, mine):
    def kernel(flag, nearh, nearl, got, cur, mine, out, tok):
        tok[0] = flag[0]

        @pl.when(flag[0] > 0)
        def _():
            w = wide(got[...])

            def mul(ds):
                out[ds] = cur[ds] - mmw(nearh[ds], nearl[ds], w)

            rows_loop(out.shape[0], mul)

        @pl.when(flag[0] == 0)
        def _():
            out[...] = mine[...]

    return pl.pallas_call(
        kernel,
        out_shape=(jax.ShapeDtypeStruct(mine.shape, F32), jax.ShapeDtypeStruct((1,), jnp.int32)),
        in_specs=[sspec(), vspec(), vspec(), vspec(), vspec(), vspec()],
        out_specs=(vspec(), sspec()),
        compiler_params=PARAMS,
        name="near",
    )(flag, nearh, nearl, got, cur, mine)


def far_call(idx, tok, hi, lo, invh, invl, acc, xb, xa):
    nb = acc.shape[0]

    def kernel(idx, tok, hi, lo, invh, invl, acc, xb, xa, acc_out, cur_out):
        @pl.when(idx[2] > 0)
        def _():
            w = jnp.concatenate([wide(xb[...]), wide(xa[...])], 0)

            def mul(ds):
                acc_out[ds] = acc[ds] - mmw(hi[ds], lo[ds], w)

            rows_loop(nb, mul)
            a = wide(acc_out[...])

            def mul2(ds):
                cur_out[ds] = mmw(invh[ds], invl[ds], a)

            rows_loop(nb, mul2)

        @pl.when(idx[2] == 0)
        def _():
            acc_out[...] = acc[...]
            cur_out[...] = acc[...]

    out = jax.ShapeDtypeStruct(acc.shape, F32)
    return pl.pallas_call(
        kernel,
        out_shape=(out, out),
        in_specs=[sspec(), sspec()] + [vspec()] * 7,
        out_specs=(vspec(), vspec()),
        compiler_params=PARAMS,
        name="far",
    )(idx, tok, hi, lo, invh, invl, acc, xb, xa)


def bulk_call(g, idx, store, acc, count):
    nb, width = acc.shape
    m = len(g.arrays)

    def kernel(idx, store, acc, *rest):
        refs = rest[:m]
        out, buf, sem = rest[m:]
        for k in range(count):
            g.start(refs, idx[k], buf.at[k], sem.at[k])
        out[...] = acc[...]

        def one(k, _):
            arrived(buf.at[k], sem.at[k])
            w = wide(store[k])

            def mul(ds):
                out[ds] = out[ds] - mmw(*split(buf[k, ds]), w)

            rows_loop(nb, mul)
            return 0

        lax.fori_loop(0, count, one, 0)

    return pl.pallas_call(
        kernel,
        out_shape=jax.ShapeDtypeStruct(acc.shape, F32),
        in_specs=[sspec(), vspec(), vspec()] + g.specs(),
        out_specs=vspec(),
        scratch_shapes=[VMEM((count, nb, nb), F32), pltpu.SemaphoreType.DMA((count,))],
        compiler_params=PARAMS,
        name="bulk",
    )(idx, store, acc, *g.arrays)


def after(x, *others):
    return lax.optimization_barrier((x,) + others)[0]


def on_device(tri_panels, rhs_rows):
    R = lax.axis_size("row")
    C = lax.axis_size("col")
    p = lax.axis_index("row")
    c = lax.axis_index("col")
    nb = tri_panels.shape[1]
    half = nb // 2
    blocks = tri_panels.shape[0] // nb
    sub = nb // C
    width = rhs_rows.shape[1] // C

    def xp(a):
        return lax.ppermute(a, "col", [(i, (i + 4) % C) for i in range(C)])

    def xm(a):
        return lax.ppermute(a, "col", [(i, (i - 4) % C) for i in range(C)])

    def yy(a):
        return lax.ppermute(a, "col", [(i, i ^ 2) for i in range(C)])

    def dd(a):
        return lax.ppermute(a, "col", [(i, i ^ 1) for i in range(C)])

    def round1(u):
        return {(0, 0): [u], (1, 0): [xp(u)], (3, 0): [xm(u)], (0, 1): [yy(u)]}

    def round2(t):
        return {(2, 0): [xp(t[1, 0][0])], (3, 1): [xm(t[0, 1][0])], (1, 1): [yy(t[1, 0][0])]}

    def round3(t):
        h = t[2, 0][0].shape[0] // 2
        return {(2, 1): [yy(t[2, 0][0][:h]), xm(t[3, 1][0][h:])]}

    def across(t):
        return {k: [dd(a) for a in v] for k, v in t.items()}

    def panels(t, d, parts):
        table = []
        for dx in range(4):
            for dy in range(2):
                table += [t[dx, dy], d[dx, dy]]
        return Panels(table, parts)

    def where_is(k):
        dx = (c // 4 - k // 4) % 4
        return dx * 4 + ((c ^ k) & 3)

    def ints(*v):
        return jnp.stack([jnp.asarray(x, jnp.int32) for x in v])

    own = tri_panels.reshape(blocks, nb, nb)
    flag = ints(c % R == p, c // R)
    own = inverse_call(flag, own)
    top, low = own[0], own[1]
    moved = lax.ppermute(top[half:], "col", [(i, i + R) for i in range(R)])
    u0 = jnp.where(c < R, top[:half], moved)

    t0 = round1(u0)
    t0.update(round2(t0))
    t0.update(round3(t0))
    d0 = across(t0)
    g0 = panels(t0, d0, 2)

    parted = rhs_rows.reshape(blocks, sub, rhs_rows.shape[1])
    state = lax.all_to_all(parted, "col", split_axis=2, concat_axis=1, tiled=True)
    acc0, acc1 = state[0], state[1]

    low = after(low, t0[2, 1][0], t0[2, 1][1])
    t1 = round1(low)
    invh, invl, nearh, nearl, cur = prep_call(g0, ints(where_is(p), where_is(jnp.maximum(p - 1, 0))), acc0)
    acc = acc0
    zero = jnp.zeros((nb, width), F32)
    store = jnp.zeros((R + 1, nb, width), F32)
    mine = jnp.where(p == 0, cur, zero)
    g = g0
    for t in range(C - 1):
        s = t % R
        with jax.named_scope(f"near{t}"):
            P1 = lax.ppermute(mine, "row", [(s, (s + 1) % R)])
        B = [((t - j) % R, (t + 2 + j) % R) for j in range(3) if t - j >= 0 and t + 2 + j < C]
        A = [((t - j) % R, (t + 1 + j) % R) for j in range(1, 4) if t - j >= 0 and t + 1 + j < C]
        with jax.named_scope(f"far{t}"):
            XB = lax.ppermute(mine, "row", B) if B else zero
            XA = lax.ppermute(mine, "row", A) if A else zero
        q = (p - t) % R
        i = t + q
        kA = i - 2 * q + 1
        kB = kA + 1
        inwin = (q >= 2) & (q <= 4)
        first = t + 1 < R
        top_k = R - 1 if first else C - 1
        fi = ints(where_is(jnp.clip(kB, 0, top_k)), where_is(jnp.clip(kA, 0, top_k)), inwin)
        turn = ints(p == (t + 1) % R)
        last_first = t + 1 == R - 1
        if t == 2:
            t1 = {k: [after(v[0], mine)] for k, v in t1.items()}
            d1 = across(t1)
            t2 = round2(t1)
        if t == 5:
            t2 = {k: [after(v[0], mine)] for k, v in t2.items()}
            d1.update(across(t2))
            t1.update(t2)
            t3 = round3(t1)
            d1.update(across(t3))
            t1.update(t3)
            g1 = panels(t1, d1, 1)
        mine, tok = near_call(turn, nearh, nearl, P1, cur, mine)
        if first:
            out0 = mine
            if B:
                store = lax.dynamic_update_index_in_dim(store, XB, jnp.where(inwin & (kB >= 0), kB, R), 0)
            if A:
                store = lax.dynamic_update_index_in_dim(store, XA, jnp.where(inwin & (kA >= 0), kA, R), 0)
            store = lax.dynamic_update_index_in_dim(store, P1, jnp.where(p == t + 1, t, R), 0)
        if last_first:
            store = lax.dynamic_update_index_in_dim(store, mine, p, 0)
            acc = bulk_call(g1, ints(*[where_is(k) for k in range(R)]), store, acc1, R)
            invh, invl, nearh, nearl, cur = prep_call(g1, ints(where_is(R + p), where_is(R + p - 1)), acc)
            g = g1
        elif B or A:
            hi, lo = pick_call(g, fi, nb)
            acc, cur = far_call(fi, tok, hi, lo, invh, invl, acc, XB, XA)
    return jnp.concatenate([out0, mine], 0)


def solution(mesh):
    return jax.shard_map(
        on_device,
        mesh=mesh,
        in_specs=(P("row", "col"), P(("row", "col"), None)),
        out_specs=P("row", "col"),
        check_vma=False,
    )
```

```python
import jax
import jax.numpy as jnp
from jax import lax
from jax.experimental import pallas as pl
from jax.experimental.pallas import tpu as pltpu
from jax.sharding import PartitionSpec as P

F32 = jnp.float32
BF16 = jnp.bfloat16
VMEM = pltpu.VMEM
SMEM = pltpu.SMEM
TILE = 256

def split(x):
    hi = x.astype(BF16)
    lo = (x - hi.astype(F32)).astype(BF16)
    return hi, lo


def left3(x):
    hi, lo = split(x)
    return jnp.concatenate([hi, hi, lo], 1)


def right3(x):
    hi, lo = split(x)
    return jnp.concatenate([hi, lo, hi], 0)


def mm3(a, b):
    return jnp.dot(left3(a), right3(b), preferred_element_type=F32)


def wide(x):
    return jnp.concatenate(split(x), 1)


def mmw(hi, lo, w):
    r = jnp.dot(hi, w, preferred_element_type=F32) + jnp.dot(lo, w, preferred_element_type=F32)
    n = w.shape[1] // 2
    return r[:, :n] + r[:, n:]


def vspec():
    return pl.BlockSpec(memory_space=VMEM)


def sspec():
    return pl.BlockSpec(memory_space=SMEM)


def aspec():
    return pl.BlockSpec(memory_space=pl.ANY)


def params(mib):
    return pltpu.CompilerParams(vmem_limit_bytes=mib * 1024 * 1024)


def rows_loop(n, body, tile=TILE):
    lax.fori_loop(0, n // tile, lambda r, _: (body(pl.ds(pl.multiple_of(r * tile, tile), tile)), 0)[1], 0)


def inverse_kernel(flag, own, out):
    nb = own.shape[1]
    h = nb // 2
    out[...] = own[...]

    def invert(slot):
        row = lax.broadcasted_iota(jnp.int32, (h, h), 0)
        col = lax.broadcasted_iota(jnp.int32, (h, h), 1)
        a0 = own[slot, :h, :h]
        a1 = own[slot, h:, h:]
        on = row == col
        y0 = jnp.where(on, 1.0 / jnp.where(on, a0, 1.0), 0.0)
        y1 = jnp.where(on, 1.0 / jnp.where(on, a1, 1.0), 0.0)

        def level(n, ys):
            y0, y1 = ys
            s = lax.shift_left(jnp.int32(1), n)
            pick = (lax.shift_right_logical(row, n + 1) == lax.shift_right_logical(col, n + 1))
            pick = pick & ((row & s) != 0) & ((col & s) == 0)
            e0 = jnp.where(pick, a0, 0.0)
            e1 = jnp.where(pick, a1, 0.0)
            z0 = mm3(e0, y0)
            z1 = mm3(e1, y1)
            return y0 - mm3(y0, z0), y1 - mm3(y1, z1)

        steps = h.bit_length() - 1
        y0, y1 = lax.fori_loop(0, steps, level, (y0, y1))
        z = mm3(own[slot, h:, :h], y0)
        out[slot, :h, :h] = y0
        out[slot, h:, h:] = y1
        out[slot, h:, :h] = -mm3(y1, z)
        out[slot, :h, h:] = jnp.zeros((h, h), F32)

    @pl.when(flag[0] > 0)
    def _():
        invert(flag[1])


def inverse_call(flag, own):
    return pl.pallas_call(
        inverse_kernel,
        out_shape=jax.ShapeDtypeStruct(own.shape, F32),
        in_specs=[sspec(), vspec()],
        out_specs=vspec(),
        compiler_params=params(20),
        name="inverse",
    )(flag, own)


def load_call(g):
    parts, count, rows, nb = g.shape

    def kernel(g, hi, lo):
        k = pl.program_id(0)
        for part in range(parts):
            for at in range(0, rows, 128):
                ds = pl.ds(part * rows + at, 128)
                hi[k, ds], lo[k, ds] = split(g[part, 0, at : at + 128])

    out = jax.ShapeDtypeStruct((count, nb, nb), BF16)
    return pl.pallas_call(
        kernel,
        out_shape=(out, out),
        grid=(count,),
        in_specs=[pl.BlockSpec((parts, 1, rows, nb), lambda k: (0, k, 0, 0))],
        out_specs=(vspec(), vspec()),
        compiler_params=params(6),
        name="load",
    )(g)


def prep_call(tab, base, hi, lo, acc):
    nb, width = acc.shape

    def kernel(tab, hi, lo, acc, nearh, nearl, cur):
        ki = tab[base]
        kn = tab[base + 1]
        w = jnp.concatenate([hi[kn], lo[kn]], 1)
        a = wide(acc[...])

        def mul(ds):
            nearh[ds], nearl[ds] = split(mmw(hi[ki, ds], lo[ki, ds], w))
            cur[ds] = mmw(hi[ki, ds], lo[ki, ds], a)

        rows_loop(nb, mul)

    sq = jax.ShapeDtypeStruct((nb, nb), BF16)
    return pl.pallas_call(
        kernel,
        out_shape=(sq, sq, jax.ShapeDtypeStruct((nb, width), F32)),
        in_specs=[sspec()] + [vspec()] * 3,
        out_specs=(vspec(),) * 3,
        compiler_params=params(8),
        name="prep",
    )(tab, hi, lo, acc)


ROW = 8


def near_call(tab, tok, nearh, nearl, got, cur, mine, store):
    keep = store is not None

    def kernel(tab, tok, nearh, nearl, got, cur, mine, *rest):
        out, tok_out = rest[-2:]
        at = tok[0] * ROW
        tok_out[0] = tok[0] + 1

        @pl.when(tab[at + 6] > 0)
        def _():
            w = wide(got[...])

            def mul(ds):
                out[ds] = cur[ds] - mmw(nearh[ds], nearl[ds], w)

            rows_loop(out.shape[0], mul)
            if keep:
                k = tab[at + 7]
                rest[1][k] = got[...]
                rest[1][k + 1] = out[...]

        @pl.when(tab[at + 6] == 0)
        def _():
            out[...] = mine[...]

    outs = [jax.ShapeDtypeStruct(mine.shape, F32), jax.ShapeDtypeStruct((1,), jnp.int32)]
    ospecs = [vspec(), sspec()]
    args = [tab, tok, nearh, nearl, got, cur, mine]
    if keep:
        outs.insert(0, jax.ShapeDtypeStruct(store.shape, F32))
        ospecs.insert(0, vspec())
        args.append(store)
    res = pl.pallas_call(
        kernel,
        out_shape=tuple(outs),
        in_specs=[sspec(), sspec()] + [vspec()] * (len(args) - 2),
        out_specs=tuple(ospecs),
        input_output_aliases={7: 0} if keep else {},
        compiler_params=params(4),
        name="near",
    )(*args)
    return res if keep else (None,) + tuple(res)


def far_call(tab, tok, hi, lo, acc, cur, xb, xa, store):
    nb = acc.shape[0]
    keep = store is not None

    def kernel(tab, tok, hi, lo, acc, cur, xb, xa, *rest):
        acc_out, cur_out = rest[-2:]
        at = (tok[0] - 1) * ROW

        @pl.when(tab[at + 2] > 0)
        def _():
            kb = tab[at + 0]
            ka = tab[at + 1]
            ki = tab[at + 5]
            wb = wide(xb[...])
            wa = wide(xa[...])

            def mul(ds):
                acc_out[ds] = acc[ds] - (mmw(hi[kb, ds], lo[kb, ds], wb) + mmw(hi[ka, ds], lo[ka, ds], wa))

            rows_loop(nb, mul)
            a = wide(acc_out[...])

            def mul2(ds):
                cur_out[ds] = mmw(hi[ki, ds], lo[ki, ds], a)

            rows_loop(nb, mul2)
            if keep:
                rest[1][tab[at + 3]] = xb[...]
                rest[1][tab[at + 4]] = xa[...]

    out = jax.ShapeDtypeStruct(acc.shape, F32)
    outs = [out, out]
    args = [tab, tok, hi, lo, acc, cur, xb, xa]
    alias = {4: 0, 5: 1}
    if keep:
        outs.insert(0, jax.ShapeDtypeStruct(store.shape, F32))
        args.append(store)
        alias = {8: 0, 4: 1, 5: 2}
    res = pl.pallas_call(
        kernel,
        out_shape=tuple(outs),
        in_specs=[sspec(), sspec()] + [vspec()] * (len(args) - 2),
        out_specs=(vspec(),) * len(outs),
        input_output_aliases=alias,
        compiler_params=params(4),
        name="far",
    )(*args)
    return res if keep else (None,) + tuple(res)


def bulk_call(tab, row, hi, lo, store, acc, xb, xa, count):
    nb, width = acc.shape

    def kernel(tab, hi, lo, store, acc, xb, xa, out, last):
        out[...] = acc[...]

        def one(k, _):
            last[...] = store[k]

            @pl.when((tab[row * ROW + 2] > 0) & (tab[row * ROW + 3] == k))
            def _():
                last[...] = xb[...]

            @pl.when((tab[row * ROW + 2] > 0) & (tab[row * ROW + 4] == k))
            def _():
                last[...] = xa[...]

            w = wide(last[...])

            def mul(ds):
                out[ds] = out[ds] - mmw(hi[k, ds], lo[k, ds], w)

            rows_loop(nb, mul)
            return 0

        lax.fori_loop(0, count, one, 0)

    return pl.pallas_call(
        kernel,
        out_shape=jax.ShapeDtypeStruct(acc.shape, F32),
        in_specs=[sspec()] + [vspec()] * 6,
        out_specs=vspec(),
        scratch_shapes=[VMEM((nb, width), F32)],
        compiler_params=params(4),
        name="bulk",
    )(tab, hi, lo, store, acc, xb, xa)


def after(x, *others):
    return lax.optimization_barrier((x,) + others)[0]


def on_device(tri_panels, rhs_rows):
    R = lax.axis_size("row")
    C = lax.axis_size("col")
    p = lax.axis_index("row")
    c = lax.axis_index("col")
    nb = tri_panels.shape[1]
    half = nb // 2
    blocks = tri_panels.shape[0] // nb
    sub = nb // C
    width = rhs_rows.shape[1] // C

    def ints(*v):
        return jnp.stack([jnp.asarray(x, jnp.int32) for x in v])

    own = tri_panels.reshape(blocks, nb, nb)
    flag = ints(c % R == p, c // R)
    own = inverse_call(flag, own)
    top, low = own[0], own[1]
    moved = lax.ppermute(top[half:], "col", [(i, i + R) for i in range(R)])
    u0 = jnp.where(c < R, top[:half], moved)

    g0 = lax.all_gather(u0, "col", axis=0, tiled=False).reshape(2, R, half, nb)
    g1 = lax.all_gather(low, "col", axis=0, tiled=False).reshape(1, C, nb, nb)

    parted = rhs_rows.reshape(blocks * sub, C, width).transpose(1, 0, 2)
    got = lax.all_to_all(parted, "col", split_axis=0, concat_axis=0, tiled=False)
    state = got.reshape(C, blocks, sub, width).transpose(1, 0, 2, 3).reshape(blocks, nb, width)
    acc, acc1 = state[0], state[1]

    rows = []
    for t in range(C - 1):
        q = (p - t) % R
        i = t + q
        kA = i - 2 * q + 1
        kB = kA + 1
        inwin = (q >= 2) & (q <= 4)
        first = t + 1 < R
        top_k = R - 1 if first else C - 1
        rows += [
            jnp.clip(kB, 0, top_k),
            jnp.clip(kA, 0, top_k),
            inwin,
            jnp.where(kB >= 0, jnp.minimum(kB, R), R),
            jnp.where(kA >= 0, jnp.minimum(kA, R), R),
            p if first else R + p,
            p == (t + 1) % R,
            min(t, R - 1),
        ]
    tab = ints(*rows, p, jnp.maximum(p - 1, 0), R + p, R + p - 1)
    hi, lo = load_call(g0)
    nearh, nearl, cur = prep_call(tab, (C - 1) * ROW, hi, lo, acc)
    zero = jnp.zeros((nb, width), F32)
    mine = jnp.where(p == 0, cur, zero)
    store = jnp.zeros((R + 1, nb, width), F32)
    store = lax.dynamic_update_index_in_dim(store, mine, 0, 0)
    tok = jnp.zeros((1,), jnp.int32)
    for t in range(C - 1):
        s = t % R
        with jax.named_scope(f"near{t}"):
            P1 = lax.ppermute(mine, "row", [(s, (s + 1) % R)])
        B = [((t - j) % R, (t + 2 + j) % R) for j in range(3) if t - j >= 0 and t + 2 + j < C]
        A = [((t - j) % R, (t + 1 + j) % R) for j in range(1, 4) if t - j >= 0 and t + 1 + j < C]
        with jax.named_scope(f"far{t}"):
            XB = lax.ppermute(mine, "row", B) if B else zero
            XA = lax.ppermute(mine, "row", A) if A else zero
        first = t + 1 < R
        store, mine, tok = near_call(tab, tok, nearh, nearl, P1, cur, mine, store if first else None)
        if first:
            out0 = mine
        if t + 1 == R - 1:
            hi, lo = load_call(g1)
            acc = bulk_call(tab, t, hi, lo, store, acc1, XB, XA, R)
            nearh, nearl, cur = prep_call(tab, (C - 1) * ROW + 2, hi, lo, acc)
        elif B or A:
            store, acc, cur = far_call(tab, tok, hi, lo, acc, cur, XB, XA, store if first else None)
    return jnp.concatenate([out0, mine], 0)


def solution(mesh):
    return jax.shard_map(
        on_device,
        mesh=mesh,
        in_specs=(P("row", "col"), P(("row", "col"), None)),
        out_specs=P("row", "col"),
        check_vma=False,
    )
```

```python
import jax
import jax.numpy as jnp
from jax import lax
from jax.experimental import pallas as pl
from jax.experimental.pallas import tpu as pltpu
from jax.sharding import PartitionSpec as P

F32 = jnp.float32
BF16 = jnp.bfloat16
VMEM = pltpu.VMEM
SMEM = pltpu.SMEM
TILE = 256

def split(x):
    hi = x.astype(BF16)
    lo = (x - hi.astype(F32)).astype(BF16)
    return hi, lo


def left3(x):
    hi, lo = split(x)
    return jnp.concatenate([hi, hi, lo], 1)


def right3(x):
    hi, lo = split(x)
    return jnp.concatenate([hi, lo, hi], 0)


def mm3(a, b):
    return jnp.dot(left3(a), right3(b), preferred_element_type=F32)


def wide(x):
    return jnp.concatenate(split(x), 1)


def mmw(hi, lo, w):
    r = jnp.dot(hi, w, preferred_element_type=F32) + jnp.dot(lo, w, preferred_element_type=F32)
    n = w.shape[1] // 2
    return r[:, :n] + r[:, n:]


def vspec():
    return pl.BlockSpec(memory_space=VMEM)


def sspec():
    return pl.BlockSpec(memory_space=SMEM)


def aspec():
    return pl.BlockSpec(memory_space=pl.ANY)


def params(mib):
    return pltpu.CompilerParams(vmem_limit_bytes=mib * 1024 * 1024)


def rows_loop(n, body, tile=TILE):
    lax.fori_loop(0, n // tile, lambda r, _: (body(pl.ds(pl.multiple_of(r * tile, tile), tile)), 0)[1], 0)


def inverse_kernel(flag, own, out):
    nb = own.shape[1]
    h = nb // 2
    out[...] = own[...]

    def invert(slot):
        row = lax.broadcasted_iota(jnp.int32, (h, h), 0)
        col = lax.broadcasted_iota(jnp.int32, (h, h), 1)
        a0 = own[slot, :h, :h]
        a1 = own[slot, h:, h:]
        on = row == col
        y0 = jnp.where(on, 1.0 / jnp.where(on, a0, 1.0), 0.0)
        y1 = jnp.where(on, 1.0 / jnp.where(on, a1, 1.0), 0.0)

        def level(n, ys):
            y0, y1 = ys
            s = lax.shift_left(jnp.int32(1), n)
            pick = (lax.shift_right_logical(row, n + 1) == lax.shift_right_logical(col, n + 1))
            pick = pick & ((row & s) != 0) & ((col & s) == 0)
            e0 = jnp.where(pick, a0, 0.0)
            e1 = jnp.where(pick, a1, 0.0)
            z0 = mm3(e0, y0)
            z1 = mm3(e1, y1)
            return y0 - mm3(y0, z0), y1 - mm3(y1, z1)

        steps = h.bit_length() - 1
        y0, y1 = lax.fori_loop(0, steps, level, (y0, y1))
        z = mm3(own[slot, h:, :h], y0)
        out[slot, :h, :h] = y0
        out[slot, h:, h:] = y1
        out[slot, h:, :h] = -mm3(y1, z)
        out[slot, :h, h:] = jnp.zeros((h, h), F32)

    @pl.when(flag[0] > 0)
    def _():
        invert(flag[1])


def inverse_call(flag, own):
    return pl.pallas_call(
        inverse_kernel,
        out_shape=jax.ShapeDtypeStruct(own.shape, F32),
        in_specs=[sspec(), vspec()],
        out_specs=vspec(),
        compiler_params=params(20),
        name="inverse",
    )(flag, own)


def load_call(g):
    parts, count, rows, nb = g.shape

    def kernel(g, hi, lo):
        k = pl.program_id(0)
        for part in range(parts):
            for at in range(0, rows, 128):
                ds = pl.ds(part * rows + at, 128)
                hi[k, ds], lo[k, ds] = split(g[part, 0, at : at + 128])

    out = jax.ShapeDtypeStruct((count, nb, nb), BF16)
    return pl.pallas_call(
        kernel,
        out_shape=(out, out),
        grid=(count,),
        in_specs=[pl.BlockSpec((parts, 1, rows, nb), lambda k: (0, k, 0, 0))],
        out_specs=(vspec(), vspec()),
        compiler_params=params(6),
        name="load",
    )(g)


def prep_call(row, hi, lo, acc):
    nb, width = acc.shape

    def kernel(row, hi, lo, acc, nearh, nearl, cur):
        ki = nth(row, 0)
        kn = nth(row, 1)
        w = jnp.concatenate([hi[kn], lo[kn]], 1)
        a = wide(acc[...])

        def mul(ds):
            nearh[ds], nearl[ds] = split(mmw(hi[ki, ds], lo[ki, ds], w))
            cur[ds] = mmw(hi[ki, ds], lo[ki, ds], a)

        rows_loop(nb, mul)

    sq = jax.ShapeDtypeStruct((nb, nb), BF16)
    return pl.pallas_call(
        kernel,
        out_shape=(sq, sq, jax.ShapeDtypeStruct((nb, width), F32)),
        in_specs=[vspec()] + [vspec()] * 3,
        out_specs=(vspec(),) * 3,
        compiler_params=params(8),
        name="prep",
    )(row, hi, lo, acc)


def nth(row, n):
    return jnp.max(row[n : n + 1, :])


def near_call(row, nearh, nearl, got, cur, mine, store):
    keep = store is not None

    def kernel(row, nearh, nearl, got, cur, mine, *rest):
        out = rest[-1]
        turn = nth(row, 6)

        @pl.when(turn > 0)
        def _():
            w = wide(got[...])

            def mul(ds):
                out[ds] = cur[ds] - mmw(nearh[ds], nearl[ds], w)

            rows_loop(out.shape[0], mul)
            if keep:
                k = nth(row, 7)
                rest[1][k] = got[...]
                rest[1][k + 1] = out[...]

        @pl.when(turn == 0)
        def _():
            out[...] = mine[...]

    outs = [jax.ShapeDtypeStruct(mine.shape, F32)]
    args = [row, nearh, nearl, got, cur, mine]
    if keep:
        outs.insert(0, jax.ShapeDtypeStruct(store.shape, F32))
        args.append(store)
    res = pl.pallas_call(
        kernel,
        out_shape=tuple(outs),
        in_specs=[vspec()] * len(args),
        out_specs=(vspec(),) * len(outs),
        input_output_aliases={6: 0} if keep else {},
        compiler_params=params(4),
        name="near",
    )(*args)
    return res if keep else (None,) + tuple(res)


def far_call(row, done, hi, lo, acc, cur, xb, xa, store):
    nb = acc.shape[0]
    keep = store is not None

    def kernel(row, done, hi, lo, acc, cur, xb, xa, *rest):
        acc_out, cur_out = rest[-2:]

        @pl.when(nth(row, 2) > 0)
        def _():
            kb = nth(row, 0)
            ka = nth(row, 1)
            ki = nth(row, 5)
            wb = wide(xb[...])
            wa = wide(xa[...])

            def mul(ds):
                acc_out[ds] = acc[ds] - (mmw(hi[kb, ds], lo[kb, ds], wb) + mmw(hi[ka, ds], lo[ka, ds], wa))

            rows_loop(nb, mul)
            a = wide(acc_out[...])

            def mul2(ds):
                cur_out[ds] = mmw(hi[ki, ds], lo[ki, ds], a)

            rows_loop(nb, mul2)
            if keep:
                rest[1][nth(row, 3)] = xb[...]
                rest[1][nth(row, 4)] = xa[...]

    out = jax.ShapeDtypeStruct(acc.shape, F32)
    outs = [out, out]
    args = [row, done, hi, lo, acc, cur, xb, xa]
    alias = {4: 0, 5: 1}
    if keep:
        outs.insert(0, jax.ShapeDtypeStruct(store.shape, F32))
        args.append(store)
        alias = {8: 0, 4: 1, 5: 2}
    res = pl.pallas_call(
        kernel,
        out_shape=tuple(outs),
        in_specs=[vspec(), aspec()] + [vspec()] * (len(args) - 2),
        out_specs=(vspec(),) * len(outs),
        input_output_aliases=alias,
        compiler_params=params(4),
        name="far",
    )(*args)
    return res if keep else (None,) + tuple(res)


def bulk_call(row, hi, lo, store, acc, xb, xa, count):
    nb, width = acc.shape

    def kernel(row, hi, lo, store, acc, xb, xa, out, last):
        out[...] = acc[...]

        def one(k, _):
            last[...] = store[k]

            @pl.when((nth(row, 2) > 0) & (nth(row, 3) == k))
            def _():
                last[...] = xb[...]

            @pl.when((nth(row, 2) > 0) & (nth(row, 4) == k))
            def _():
                last[...] = xa[...]

            w = wide(last[...])

            def mul(ds):
                out[ds] = out[ds] - mmw(hi[k, ds], lo[k, ds], w)

            rows_loop(nb, mul)
            return 0

        lax.fori_loop(0, count, one, 0)

    return pl.pallas_call(
        kernel,
        out_shape=jax.ShapeDtypeStruct(acc.shape, F32),
        in_specs=[vspec()] + [vspec()] * 6,
        out_specs=vspec(),
        scratch_shapes=[VMEM((nb, width), F32)],
        compiler_params=params(4),
        name="bulk",
    )(row, hi, lo, store, acc, xb, xa)


def after(x, *others):
    return lax.optimization_barrier((x,) + others)[0]


def on_device(tri_panels, rhs_rows):
    R = lax.axis_size("row")
    C = lax.axis_size("col")
    p = lax.axis_index("row")
    c = lax.axis_index("col")
    nb = tri_panels.shape[1]
    half = nb // 2
    blocks = tri_panels.shape[0] // nb
    sub = nb // C
    width = rhs_rows.shape[1] // C

    def ints(*v):
        return jnp.stack([jnp.asarray(x, jnp.int32) for x in v])

    own = tri_panels.reshape(blocks, nb, nb)
    flag = ints(c % R == p, c // R)
    own = inverse_call(flag, own)
    top, low = own[0], own[1]
    moved = lax.ppermute(top[half:], "col", [(i, i + R) for i in range(R)])
    u0 = jnp.where(c < R, top[:half], moved)

    g0 = lax.all_gather(u0, "col", axis=0, tiled=False).reshape(2, R, half, nb)
    g1 = lax.all_gather(low, "col", axis=0, tiled=False).reshape(1, C, nb, nb)

    parted = rhs_rows.reshape(blocks * sub, C, width).transpose(1, 0, 2)
    got = lax.all_to_all(parted, "col", split_axis=0, concat_axis=0, tiled=False)
    state = got.reshape(C, blocks, sub, width).transpose(1, 0, 2, 3).reshape(blocks, nb, width)
    acc, acc1 = state[0], state[1]

    def sublanes(*v):
        v = v + (0,) * (8 - len(v))
        return jnp.broadcast_to(ints(*v)[:, None], (8, 128))

    rows = []
    for t in range(C - 1):
        q = (p - t) % R
        i = t + q
        kA = i - 2 * q + 1
        kB = kA + 1
        inwin = (q >= 2) & (q <= 4)
        first = t + 1 < R
        top_k = R - 1 if first else C - 1
        rows.append(sublanes(
            jnp.clip(kB, 0, top_k),
            jnp.clip(kA, 0, top_k),
            inwin,
            jnp.where(kB >= 0, jnp.minimum(kB, R), R),
            jnp.where(kA >= 0, jnp.minimum(kA, R), R),
            p if first else R + p,
            p == (t + 1) % R,
            min(t, R - 1),
        ))
    rows += [sublanes(p, jnp.maximum(p - 1, 0)), sublanes(R + p, R + p - 1)]
    hi, lo = load_call(g0)
    rows = lax.optimization_barrier(tuple(rows) + (acc,))
    acc = rows[-1]
    nearh, nearl, cur = prep_call(rows[C - 1], hi, lo, acc)
    zero = jnp.zeros((nb, width), F32)
    mine = jnp.where(p == 0, cur, zero)
    store = jnp.zeros((R + 1, nb, width), F32)
    store = lax.dynamic_update_index_in_dim(store, mine, 0, 0)
    for t in range(C - 1):
        s = t % R
        with jax.named_scope(f"near{t}"):
            P1 = lax.ppermute(mine, "row", [(s, (s + 1) % R)])
        B = [((t - j) % R, (t + 2 + j) % R) for j in range(3) if t - j >= 0 and t + 2 + j < C]
        A = [((t - j) % R, (t + 1 + j) % R) for j in range(1, 4) if t - j >= 0 and t + 1 + j < C]
        with jax.named_scope(f"far{t}"):
            XB = lax.ppermute(mine, "row", B) if B else zero
            XA = lax.ppermute(mine, "row", A) if A else zero
        first = t + 1 < R
        store, mine = near_call(rows[t], nearh, nearl, P1, cur, mine, store if first else None)
        if first:
            out0 = mine
        if t + 1 == R - 1:
            hi, lo = load_call(g1)
            acc = bulk_call(rows[t], hi, lo, store, acc1, XB, XA, R)
            nearh, nearl, cur = prep_call(rows[C], hi, lo, acc)
        elif B or A:
            store, acc, cur = far_call(rows[t], mine, hi, lo, acc, cur, XB, XA, store if first else None)
    return jnp.concatenate([out0, mine], 0)


def solution(mesh):
    return jax.shard_map(
        on_device,
        mesh=mesh,
        in_specs=(P("row", "col"), P(("row", "col"), None)),
        out_specs=P("row", "col"),
        check_vma=False,
    )
```

```python
import jax
import jax.numpy as jnp
from jax import lax
from jax.experimental import pallas as pl
from jax.experimental.pallas import tpu as pltpu
from jax.sharding import PartitionSpec as P

F32 = jnp.float32
BF16 = jnp.bfloat16
VMEM = pltpu.VMEM
SMEM = pltpu.SMEM
TILE = 256

def split(x):
    hi = x.astype(BF16)
    lo = (x - hi.astype(F32)).astype(BF16)
    return hi, lo


def left3(x):
    hi, lo = split(x)
    return jnp.concatenate([hi, hi, lo], 1)


def right3(x):
    hi, lo = split(x)
    return jnp.concatenate([hi, lo, hi], 0)


def mm3(a, b):
    return jnp.dot(left3(a), right3(b), preferred_element_type=F32)


def wide(x):
    return jnp.concatenate(split(x), 1)


def mmw(hi, lo, w):
    r = jnp.dot(hi, w, preferred_element_type=F32) + jnp.dot(lo, w, preferred_element_type=F32)
    n = w.shape[1] // 2
    return r[:, :n] + r[:, n:]


def vspec():
    return pl.BlockSpec(memory_space=VMEM)


def sspec():
    return pl.BlockSpec(memory_space=SMEM)


def aspec():
    return pl.BlockSpec(memory_space=pl.ANY)


def params(mib):
    return pltpu.CompilerParams(vmem_limit_bytes=mib * 1024 * 1024)


def rows_loop(n, body, tile=TILE):
    lax.fori_loop(0, n // tile, lambda r, _: (body(pl.ds(pl.multiple_of(r * tile, tile), tile)), 0)[1], 0)


def inverse_kernel(flag, own, out):
    nb = own.shape[1]
    h = nb // 2
    out[...] = own[...]

    def invert(slot):
        row = lax.broadcasted_iota(jnp.int32, (h, h), 0)
        col = lax.broadcasted_iota(jnp.int32, (h, h), 1)
        a0 = own[slot, :h, :h]
        a1 = own[slot, h:, h:]
        on = row == col
        y0 = jnp.where(on, 1.0 / jnp.where(on, a0, 1.0), 0.0)
        y1 = jnp.where(on, 1.0 / jnp.where(on, a1, 1.0), 0.0)

        def level(n, ys):
            y0, y1 = ys
            s = lax.shift_left(jnp.int32(1), n)
            pick = (lax.shift_right_logical(row, n + 1) == lax.shift_right_logical(col, n + 1))
            pick = pick & ((row & s) != 0) & ((col & s) == 0)
            e0 = jnp.where(pick, a0, 0.0)
            e1 = jnp.where(pick, a1, 0.0)
            z0 = mm3(e0, y0)
            z1 = mm3(e1, y1)
            return y0 - mm3(y0, z0), y1 - mm3(y1, z1)

        steps = h.bit_length() - 1
        y0, y1 = lax.fori_loop(0, steps, level, (y0, y1))
        z = mm3(own[slot, h:, :h], y0)
        out[slot, :h, :h] = y0
        out[slot, h:, h:] = y1
        out[slot, h:, :h] = -mm3(y1, z)
        out[slot, :h, h:] = jnp.zeros((h, h), F32)

    @pl.when(flag[0] > 0)
    def _():
        invert(flag[1])


def inverse_call(flag, own):
    return pl.pallas_call(
        inverse_kernel,
        out_shape=jax.ShapeDtypeStruct(own.shape, F32),
        in_specs=[sspec(), vspec()],
        out_specs=vspec(),
        compiler_params=params(20),
        name="inverse",
    )(flag, own)


def load_call(g):
    parts, count, rows, nb = g.shape

    def kernel(g, hi, lo):
        k = pl.program_id(0)
        for part in range(parts):
            for at in range(0, rows, 128):
                ds = pl.ds(part * rows + at, 128)
                hi[k, ds], lo[k, ds] = split(g[part, 0, at : at + 128])

    out = jax.ShapeDtypeStruct((count, nb, nb), BF16)
    return pl.pallas_call(
        kernel,
        out_shape=(out, out),
        grid=(count,),
        in_specs=[pl.BlockSpec((parts, 1, rows, nb), lambda k: (0, k, 0, 0))],
        out_specs=(vspec(), vspec()),
        compiler_params=params(6),
        name="load",
    )(g)


def prep_call(row, hi, lo, acc):
    nb, width = acc.shape

    def kernel(row, hi, lo, acc, nearh, nearl, cur):
        ki = nth(row, 0)
        kn = nth(row, 1)
        w = jnp.concatenate([hi[kn], lo[kn]], 1)
        a = wide(acc[...])

        def mul(ds):
            nearh[ds], nearl[ds] = split(mmw(hi[ki, ds], lo[ki, ds], w))
            cur[ds] = mmw(hi[ki, ds], lo[ki, ds], a)

        rows_loop(nb, mul)

    sq = jax.ShapeDtypeStruct((nb, nb), BF16)
    return pl.pallas_call(
        kernel,
        out_shape=(sq, sq, jax.ShapeDtypeStruct((nb, width), F32)),
        in_specs=[vspec()] + [vspec()] * 3,
        out_specs=(vspec(),) * 3,
        compiler_params=params(8),
        name="prep",
    )(row, hi, lo, acc)


def nth(row, n):
    return jnp.max(row[n : n + 1, :])


def near_call(row, nearh, nearl, got, cur, mine, store):
    keep = store is not None

    def kernel(row, nearh, nearl, got, cur, mine, *rest):
        out = rest[-1]
        turn = nth(row, 6)

        @pl.when(turn > 0)
        def _():
            w = wide(got[...])

            def mul(ds):
                out[ds] = cur[ds] - mmw(nearh[ds], nearl[ds], w)

            rows_loop(out.shape[0], mul, out.shape[0])
            if keep:
                k = nth(row, 7)
                rest[1][k] = got[...]
                rest[1][k + 1] = out[...]

        @pl.when(turn == 0)
        def _():
            out[...] = mine[...]

    outs = [jax.ShapeDtypeStruct(mine.shape, F32)]
    args = [row, nearh, nearl, got, cur, mine]
    if keep:
        outs.insert(0, jax.ShapeDtypeStruct(store.shape, F32))
        args.append(store)
    res = pl.pallas_call(
        kernel,
        out_shape=tuple(outs),
        in_specs=[vspec()] * len(args),
        out_specs=(vspec(),) * len(outs),
        input_output_aliases={6: 0} if keep else {},
        compiler_params=params(4),
        name="near",
    )(*args)
    return res if keep else (None,) + tuple(res)


def far_call(row, done, hi, lo, acc, cur, xb, xa, store):
    nb = acc.shape[0]
    keep = store is not None

    def kernel(row, done, hi, lo, acc, cur, xb, xa, *rest):
        acc_out, cur_out = rest[-2:]

        @pl.when(nth(row, 2) > 0)
        def _():
            kb = nth(row, 0)
            ka = nth(row, 1)
            ki = nth(row, 5)
            wb = wide(xb[...])
            wa = wide(xa[...])

            def mul(ds):
                acc_out[ds] = acc[ds] - (mmw(hi[kb, ds], lo[kb, ds], wb) + mmw(hi[ka, ds], lo[ka, ds], wa))

            rows_loop(nb, mul)
            a = wide(acc_out[...])

            def mul2(ds):
                cur_out[ds] = mmw(hi[ki, ds], lo[ki, ds], a)

            rows_loop(nb, mul2)
            if keep:
                rest[1][nth(row, 3)] = xb[...]
                rest[1][nth(row, 4)] = xa[...]

    out = jax.ShapeDtypeStruct(acc.shape, F32)
    outs = [out, out]
    args = [row, done, hi, lo, acc, cur, xb, xa]
    alias = {4: 0, 5: 1}
    if keep:
        outs.insert(0, jax.ShapeDtypeStruct(store.shape, F32))
        args.append(store)
        alias = {8: 0, 4: 1, 5: 2}
    res = pl.pallas_call(
        kernel,
        out_shape=tuple(outs),
        in_specs=[vspec(), aspec()] + [vspec()] * (len(args) - 2),
        out_specs=(vspec(),) * len(outs),
        input_output_aliases=alias,
        compiler_params=params(4),
        name="far",
    )(*args)
    return res if keep else (None,) + tuple(res)


def bulk_call(row, hi, lo, store, acc, xb, xa, count):
    nb, width = acc.shape

    def kernel(row, hi, lo, store, acc, xb, xa, out, last):
        out[...] = acc[...]
        fresh = nth(row, 2) > 0
        kb = nth(row, 3)
        ka = nth(row, 4)

        def one(k, _):
            last[...] = store[k]

            @pl.when(fresh & (kb == k))
            def _():
                last[...] = xb[...]

            @pl.when(fresh & (ka == k))
            def _():
                last[...] = xa[...]

            w = wide(last[...])

            def mul(ds):
                out[ds] = out[ds] - mmw(hi[k, ds], lo[k, ds], w)

            rows_loop(nb, mul, nb)
            return 0

        lax.fori_loop(0, count, one, 0)

    return pl.pallas_call(
        kernel,
        out_shape=jax.ShapeDtypeStruct(acc.shape, F32),
        in_specs=[vspec()] + [vspec()] * 6,
        out_specs=vspec(),
        scratch_shapes=[VMEM((nb, width), F32)],
        compiler_params=params(4),
        name="bulk",
    )(row, hi, lo, store, acc, xb, xa)


def after(x, *others):
    return lax.optimization_barrier((x,) + others)[0]


def on_device(tri_panels, rhs_rows):
    R = lax.axis_size("row")
    C = lax.axis_size("col")
    p = lax.axis_index("row")
    c = lax.axis_index("col")
    nb = tri_panels.shape[1]
    half = nb // 2
    blocks = tri_panels.shape[0] // nb
    sub = nb // C
    width = rhs_rows.shape[1] // C

    def ints(*v):
        return jnp.stack([jnp.asarray(x, jnp.int32) for x in v])

    own = tri_panels.reshape(blocks, nb, nb)
    flag = ints(c % R == p, c // R)
    own = inverse_call(flag, own)
    top, low = own[0], own[1]
    moved = lax.ppermute(top[half:], "col", [(i, i + R) for i in range(R)])
    u0 = jnp.where(c < R, top[:half], moved)

    g0 = lax.all_gather(u0, "col", axis=0, tiled=False).reshape(2, R, half, nb)
    g1 = lax.all_gather(low, "col", axis=0, tiled=False).reshape(1, C, nb, nb)

    parted = rhs_rows.reshape(blocks * sub, C, width).transpose(1, 0, 2)
    got = lax.all_to_all(parted, "col", split_axis=0, concat_axis=0, tiled=False)
    state = got.reshape(C, blocks, sub, width).transpose(1, 0, 2, 3).reshape(blocks, nb, width)
    acc, acc1 = state[0], state[1]

    def sublanes(*v):
        v = v + (0,) * (8 - len(v))
        return jnp.broadcast_to(ints(*v)[:, None], (8, 128))

    rows = []
    for t in range(C - 1):
        q = (p - t) % R
        i = t + q
        kB = i - 2 * q + 2
        kA = kB + 1
        inwin = (q >= 2) & (q <= 5)
        first = t + 1 < R
        top_k = R - 1 if first else C - 1
        rows.append(sublanes(
            jnp.clip(kB, 0, top_k),
            jnp.clip(kA, 0, top_k),
            inwin,
            jnp.where((kB >= 0) & (q <= 4), jnp.minimum(kB, R), R),
            jnp.where((kA >= 0) & (q >= 3), jnp.minimum(kA, R), R),
            p if first else R + p,
            p == (t + 1) % R,
            min(t, R - 1),
        ))
    rows += [sublanes(p, jnp.maximum(p - 1, 0)), sublanes(R + p, R + p - 1)]
    hi, lo = load_call(g0)
    rows = lax.optimization_barrier(tuple(rows) + (acc,))
    acc = rows[-1]
    nearh, nearl, cur = prep_call(rows[C - 1], hi, lo, acc)
    zero = jnp.zeros((nb, width), F32)
    mine = jnp.where(p == 0, cur, zero)
    store = jnp.zeros((R + 1, nb, width), F32)
    store = lax.dynamic_update_index_in_dim(store, mine, 0, 0)
    for t in range(C - 1):
        s = t % R
        with jax.named_scope(f"near{t}"):
            P1 = lax.ppermute(mine, "row", [(s, (s + 1) % R)])
        B = [((t - j) % R, (t + 2 + j) % R) for j in range(3) if t - j >= 0 and t + 2 + j < C]
        A = [((t - j) % R, (t + 3 + j) % R) for j in range(3) if t - j >= 0 and t + 3 + j < C]
        with jax.named_scope(f"far{t}"):
            XB = lax.ppermute(mine, "row", B) if B else zero
            XA = lax.ppermute(mine, "row", A) if A else zero
        first = t + 1 < R
        store, mine = near_call(rows[t], nearh, nearl, P1, cur, mine, store if first else None)
        if first:
            out0 = mine
        if t + 1 == R - 1:
            hi, lo = load_call(g1)
            acc = bulk_call(rows[t], hi, lo, store, acc1, XB, XA, R)
            nearh, nearl, cur = prep_call(rows[C], hi, lo, acc)
        elif B or A:
            store, acc, cur = far_call(rows[t], mine, hi, lo, acc, cur, XB, XA, store if first else None)
    return jnp.concatenate([out0, mine], 0)


def solution(mesh):
    return jax.shard_map(
        on_device,
        mesh=mesh,
        in_specs=(P("row", "col"), P(("row", "col"), None)),
        out_specs=P("row", "col"),
        check_vma=False,
    )
```

```python
import jax
import jax.numpy as jnp
from jax import lax
from jax.experimental import pallas as pl
from jax.experimental.pallas import tpu as pltpu
from jax.sharding import PartitionSpec as P

F32 = jnp.float32
BF16 = jnp.bfloat16
VMEM = pltpu.VMEM
SMEM = pltpu.SMEM
TILE = 256

def split(x):
    hi = x.astype(BF16)
    lo = (x - hi.astype(F32)).astype(BF16)
    return hi, lo


def left3(x):
    hi, lo = split(x)
    return jnp.concatenate([hi, hi, lo], 1)


def right3(x):
    hi, lo = split(x)
    return jnp.concatenate([hi, lo, hi], 0)


def mm3(a, b):
    return jnp.dot(left3(a), right3(b), preferred_element_type=F32)


def wide(x):
    return jnp.concatenate(split(x), 1)


def mmw(hi, lo, w):
    r = jnp.dot(hi, w, preferred_element_type=F32) + jnp.dot(lo, w, preferred_element_type=F32)
    n = w.shape[1] // 2
    return r[:, :n] + r[:, n:]


def vspec():
    return pl.BlockSpec(memory_space=VMEM)


def sspec():
    return pl.BlockSpec(memory_space=SMEM)


def aspec():
    return pl.BlockSpec(memory_space=pl.ANY)


def params(mib):
    return pltpu.CompilerParams(vmem_limit_bytes=mib * 1024 * 1024)


def rows_loop(n, body, tile=TILE):
    lax.fori_loop(0, n // tile, lambda r, _: (body(pl.ds(pl.multiple_of(r * tile, tile), tile)), 0)[1], 0)


def inverse_kernel(flag, own, out):
    nb = own.shape[1]
    h = nb // 2
    out[...] = own[...]

    def invert(slot):
        row = lax.broadcasted_iota(jnp.int32, (h, h), 0)
        col = lax.broadcasted_iota(jnp.int32, (h, h), 1)
        a0 = own[slot, :h, :h]
        a1 = own[slot, h:, h:]
        on = row == col
        y0 = jnp.where(on, 1.0 / jnp.where(on, a0, 1.0), 0.0)
        y1 = jnp.where(on, 1.0 / jnp.where(on, a1, 1.0), 0.0)

        def level(n, ys):
            y0, y1 = ys
            s = lax.shift_left(jnp.int32(1), n)
            pick = (lax.shift_right_logical(row, n + 1) == lax.shift_right_logical(col, n + 1))
            pick = pick & ((row & s) != 0) & ((col & s) == 0)
            e0 = jnp.where(pick, a0, 0.0)
            e1 = jnp.where(pick, a1, 0.0)
            z0 = mm3(e0, y0)
            z1 = mm3(e1, y1)
            return y0 - mm3(y0, z0), y1 - mm3(y1, z1)

        steps = h.bit_length() - 1
        y0, y1 = lax.fori_loop(0, steps, level, (y0, y1))
        z = mm3(own[slot, h:, :h], y0)
        out[slot, :h, :h] = y0
        out[slot, h:, h:] = y1
        out[slot, h:, :h] = -mm3(y1, z)
        out[slot, :h, h:] = jnp.zeros((h, h), F32)

    @pl.when(flag[0] > 0)
    def _():
        invert(flag[1])


def inverse_call(flag, own):
    return pl.pallas_call(
        inverse_kernel,
        out_shape=jax.ShapeDtypeStruct(own.shape, F32),
        in_specs=[sspec(), vspec()],
        out_specs=vspec(),
        compiler_params=params(20),
        name="inverse",
    )(flag, own)


def load_call(g):
    parts, count, rows, nb = g.shape

    def kernel(g, hi, lo):
        k = pl.program_id(0)
        for part in range(parts):
            for at in range(0, rows, 128):
                ds = pl.ds(part * rows + at, 128)
                hi[k, ds], lo[k, ds] = split(g[part, 0, at : at + 128])

    out = jax.ShapeDtypeStruct((count, nb, nb), BF16)
    return pl.pallas_call(
        kernel,
        out_shape=(out, out),
        grid=(count,),
        in_specs=[pl.BlockSpec((parts, 1, rows, nb), lambda k: (0, k, 0, 0))],
        out_specs=(vspec(), vspec()),
        compiler_params=params(6),
        name="load",
    )(g)


def prep_call(row, hi, lo, acc):
    nb, width = acc.shape

    def kernel(row, hi, lo, acc, nearh, nearl, cur):
        ki = nth(row, 0)
        kn = nth(row, 1)
        w = jnp.concatenate([hi[kn], lo[kn]], 1)
        a = wide(acc[...])

        def mul(ds):
            nearh[ds], nearl[ds] = split(mmw(hi[ki, ds], lo[ki, ds], w))
            cur[ds] = mmw(hi[ki, ds], lo[ki, ds], a)

        rows_loop(nb, mul)

    sq = jax.ShapeDtypeStruct((nb, nb), BF16)
    return pl.pallas_call(
        kernel,
        out_shape=(sq, sq, jax.ShapeDtypeStruct((nb, width), F32)),
        in_specs=[vspec()] + [vspec()] * 3,
        out_specs=(vspec(),) * 3,
        compiler_params=params(8),
        name="prep",
    )(row, hi, lo, acc)


def nth(row, n):
    return jnp.max(row[n : n + 1, :])


def near_call(row, nearh, nearl, got, cur, mine, store):
    keep = store is not None

    def kernel(row, nearh, nearl, got, cur, mine, *rest):
        out = rest[-1]
        turn = nth(row, 6)

        @pl.when(turn > 0)
        def _():
            w = wide(got[...])

            def mul(ds):
                out[ds] = cur[ds] - mmw(nearh[ds], nearl[ds], w)

            rows_loop(out.shape[0], mul, out.shape[0])
            if keep:
                k = nth(row, 7)
                rest[1][k] = got[...]
                rest[1][k + 1] = out[...]

        @pl.when(turn == 0)
        def _():
            out[...] = mine[...]

    outs = [jax.ShapeDtypeStruct(mine.shape, F32)]
    args = [row, nearh, nearl, got, cur, mine]
    if keep:
        outs.insert(0, jax.ShapeDtypeStruct(store.shape, F32))
        args.append(store)
    res = pl.pallas_call(
        kernel,
        out_shape=tuple(outs),
        in_specs=[vspec()] * len(args),
        out_specs=(vspec(),) * len(outs),
        input_output_aliases={6: 0} if keep else {},
        compiler_params=params(4),
        name="near",
    )(*args)
    return res if keep else (None,) + tuple(res)


def far_call(row, done, hi, lo, acc, cur, xb, xa, store):
    nb = acc.shape[0]
    keep = store is not None

    def kernel(row, done, hi, lo, acc, cur, xb, xa, *rest):
        acc_out, cur_out = rest[-2:]

        ahead = nth(row, 2)

        @pl.when(ahead > 0)
        def _():
            kb = nth(row, 0)
            ka = nth(row, 1)
            ki = nth(row, 5)
            wb = wide(xb[...])
            wa = wide(xa[...])

            @pl.when(ahead == 2)
            def _():
                def mul(ds):
                    acc_out[ds] = acc[ds] - mmw(hi[kb, ds], lo[kb, ds], wb)

                rows_loop(nb, mul)

            @pl.when(ahead > 2)
            def _():
                def mul(ds):
                    acc_out[ds] = acc[ds] - (mmw(hi[kb, ds], lo[kb, ds], wb) + mmw(hi[ka, ds], lo[ka, ds], wa))

                rows_loop(nb, mul)

            a = wide(acc_out[...])

            def mul2(ds):
                cur_out[ds] = mmw(hi[ki, ds], lo[ki, ds], a)

            rows_loop(nb, mul2)
            if keep:
                rest[1][nth(row, 3)] = xb[...]
                rest[1][nth(row, 4)] = xa[...]

    out = jax.ShapeDtypeStruct(acc.shape, F32)
    outs = [out, out]
    args = [row, done, hi, lo, acc, cur, xb, xa]
    alias = {4: 0, 5: 1}
    if keep:
        outs.insert(0, jax.ShapeDtypeStruct(store.shape, F32))
        args.append(store)
        alias = {8: 0, 4: 1, 5: 2}
    res = pl.pallas_call(
        kernel,
        out_shape=tuple(outs),
        in_specs=[vspec(), aspec()] + [vspec()] * (len(args) - 2),
        out_specs=(vspec(),) * len(outs),
        input_output_aliases=alias,
        compiler_params=params(4),
        name="far",
    )(*args)
    return res if keep else (None,) + tuple(res)


def bulk_call(row, hi, lo, store, acc, xb, xa, count):
    nb, width = acc.shape

    def kernel(row, hi, lo, store, acc, xb, xa, out, last):
        out[...] = acc[...]
        fresh = nth(row, 2) > 0
        kb = nth(row, 3)
        ka = nth(row, 4)

        def one(k, _):
            last[...] = store[k]

            @pl.when(fresh & (kb == k))
            def _():
                last[...] = xb[...]

            @pl.when(fresh & (ka == k))
            def _():
                last[...] = xa[...]

            w = wide(last[...])

            def mul(ds):
                out[ds] = out[ds] - mmw(hi[k, ds], lo[k, ds], w)

            rows_loop(nb, mul, nb)
            return 0

        lax.fori_loop(0, count, one, 0)

    return pl.pallas_call(
        kernel,
        out_shape=jax.ShapeDtypeStruct(acc.shape, F32),
        in_specs=[vspec()] + [vspec()] * 6,
        out_specs=vspec(),
        scratch_shapes=[VMEM((nb, width), F32)],
        compiler_params=params(4),
        name="bulk",
    )(row, hi, lo, store, acc, xb, xa)


def after(x, *others):
    return lax.optimization_barrier((x,) + others)[0]


def on_device(tri_panels, rhs_rows):
    R = lax.axis_size("row")
    C = lax.axis_size("col")
    p = lax.axis_index("row")
    c = lax.axis_index("col")
    nb = tri_panels.shape[1]
    half = nb // 2
    blocks = tri_panels.shape[0] // nb
    sub = nb // C
    width = rhs_rows.shape[1] // C

    def ints(*v):
        return jnp.stack([jnp.asarray(x, jnp.int32) for x in v])

    own = tri_panels.reshape(blocks, nb, nb)
    flag = ints(c % R == p, c // R)
    own = inverse_call(flag, own)
    top, low = own[0], own[1]
    moved = lax.ppermute(top[half:], "col", [(i, i + R) for i in range(R)])
    u0 = jnp.where(c < R, top[:half], moved)

    g0 = lax.all_gather(u0, "col", axis=0, tiled=False).reshape(2, R, half, nb)
    g1 = lax.all_gather(low, "col", axis=0, tiled=False).reshape(1, C, nb, nb)

    parted = rhs_rows.reshape(blocks * sub, C, width).transpose(1, 0, 2)
    got = lax.all_to_all(parted, "col", split_axis=0, concat_axis=0, tiled=False)
    state = got.reshape(C, blocks, sub, width).transpose(1, 0, 2, 3).reshape(blocks, nb, width)
    acc, acc1 = state[0], state[1]

    def sublanes(*v):
        v = v + (0,) * (8 - len(v))
        return jnp.broadcast_to(ints(*v)[:, None], (8, 128))

    rows = []
    for t in range(C - 1):
        q = (p - t) % R
        i = t + q
        kB = i - 2 * q + 2
        kA = kB + 1
        inwin = jnp.where((q >= 2) & (q <= 5), q, 0)
        first = t + 1 < R
        top_k = R - 1 if first else C - 1
        rows.append(sublanes(
            jnp.clip(kB, 0, top_k),
            jnp.clip(kA, 0, top_k),
            inwin,
            jnp.where((kB >= 0) & (q <= 4), jnp.minimum(kB, R), R),
            jnp.where((kA >= 0) & (q >= 3), jnp.minimum(kA, R), R),
            p if first else R + p,
            p == (t + 1) % R,
            min(t, R - 1),
        ))
    rows += [sublanes(p, jnp.maximum(p - 1, 0)), sublanes(R + p, R + p - 1)]
    hi, lo = load_call(g0)
    rows = lax.optimization_barrier(tuple(rows) + (acc,))
    acc = rows[-1]
    nearh, nearl, cur = prep_call(rows[C - 1], hi, lo, acc)
    zero = jnp.zeros((nb, width), F32)
    mine = jnp.where(p == 0, cur, zero)
    store = jnp.zeros((R + 1, nb, width), F32)
    store = lax.dynamic_update_index_in_dim(store, mine, 0, 0)
    for t in range(C - 1):
        s = t % R
        with jax.named_scope(f"near{t}"):
            P1 = lax.ppermute(mine, "row", [(s, (s + 1) % R)])
        B = [((t - j) % R, (t + 2 + j) % R) for j in range(3) if t - j >= 0 and t + 2 + j < C]
        A = [((t - j) % R, (t + 3 + j) % R) for j in range(3) if t - j >= 0 and t + 3 + j < C]
        with jax.named_scope(f"far{t}"):
            XB = lax.ppermute(mine, "row", B) if B else zero
            XA = lax.ppermute(mine, "row", A) if A else zero
        first = t + 1 < R
        store, mine = near_call(rows[t], nearh, nearl, P1, cur, mine, store if first else None)
        if first:
            out0 = mine
        if t + 1 == R - 1:
            hi, lo = load_call(g1)
            acc = bulk_call(rows[t], hi, lo, store, acc1, XB, XA, R)
            nearh, nearl, cur = prep_call(rows[C], hi, lo, acc)
        elif B or A:
            store, acc, cur = far_call(rows[t], mine, hi, lo, acc, cur, XB, XA, store if first else None)
    return jnp.concatenate([out0, mine], 0)


def solution(mesh):
    return jax.shard_map(
        on_device,
        mesh=mesh,
        in_specs=(P("row", "col"), P(("row", "col"), None)),
        out_specs=P("row", "col"),
        check_vma=False,
    )
```
